32 devices in a mesh: rows: 8 (over z, y), cols: 4 (over x, core).
Axes of the slice: x: 2, y: 2, z: 4, core: 2. Of those that a mesh axis runs over, the one named last changes fastest.
Arguments:
- points: bfloat16 [4096, 256], P(('rows', 'cols')), may hold values from -6 to 6
- start_vectors: float32 [8, 4096], P(None, ('rows', 'cols')), may hold values from -6 to 6
- degree: bfloat16 [4096], P(('rows', 'cols')), may hold values from 0.19921875 to 2
Outputs:
- embedding: float32 [8, 4096], P(None, ('rows', 'cols'))
The draws below stay inside these ranges and needn't reach their ends.
All inputs are finite; a program needn't handle non-finite values.
Results may differ from the reference program's by a relative error of at most 0.0034.
Values may be sent and summed in bfloat16 or wider, within the bound.
No kernel may reach another device: no remote copies, remote signals or barrier semaphores. Data moves between devices by JAX's collectives and lax.ppermute only.
A program may use at most 64 MiB of HBM per device.

```python
import math
import jax
import jax.numpy as jnp
from jax import lax

F = 256
K = 8
ITERS = 3
NPTS = 4096


def draw_points(key, part):
    group_size = 16
    clusters = max(NPTS // group_size, 2)
    jitter_sq = 0.5
    centre_sq = math.log(max(NPTS - group_size, 2 * group_size) / (group_size - 1.0)) / 8.0
    key_centre = jax.random.fold_in(key, 11)
    key_label = jax.random.fold_in(key, 12)
    key_jitter = jax.random.fold_in(key, 13)
    labels = jax.random.randint(key_label, (NPTS,), 0, clusters)
    centres = jax.random.normal(key_centre, (clusters, F), jnp.float32) * math.sqrt(centre_sq)
    jitter = jax.random.normal(key_jitter, (NPTS, F), jnp.float32) * math.sqrt(jitter_sq)
    values = centres[labels] + jitter
    return jnp.clip(values, -6.0, 6.0).astype(jnp.bfloat16)


def levels(rng, dims, split, least, top_value):
    gain, own = 1.0, jax.random.fold_in(rng, 6)
    for axis_at, parts in split:
        steps = jnp.exp(jax.random.uniform(jax.random.fold_in(own, axis_at), (parts,), jnp.float32, least / len(split), top_value / len(split)))
        gain = gain * jnp.repeat(steps, dims[axis_at] // parts).reshape([-1 if axis == axis_at else 1 for axis in range(len(dims))])
    return gain


def scatter_about(rng, shape, scale, bound, shards=(), kind=jnp.bfloat16):
    factor_of = levels(rng, shape, shards, -0.22, 0.18) if shards else 1.0
    entries = jax.random.normal(rng, shape, jnp.float32) * scale * factor_of
    return jnp.minimum(jnp.maximum(entries, -bound), bound).astype(kind)


def setup_inputs(seed: int = 0) -> dict:
    streams_of = jax.random.split(jax.random.key(seed), 4)
    return {
        "points": draw_points(jax.random.fold_in(streams_of[3], 71), 0),
        "start_vectors": scatter_about(streams_of[1], (K, NPTS), 1.0, 6.0, ((1, 32),), jnp.float32),
        "degree": jnp.clip(jnp.exp(math.log(2.0) - 2.306499 * jax.random.uniform(streams_of[2], (NPTS,), jnp.float32) ** levels(streams_of[2], (NPTS,), ((0, 32),), -0.2, 0.2)), 0.19921875, 2.0).astype(jnp.bfloat16),
    }


def reference(points, start_vectors, degree):
    npts = points.shape[0]
    sharpness = 4.0 / points.shape[1]
    points_f = points.astype(jnp.float32)
    sqnorm = jnp.sum(points_f * points_f, axis=1)
    block_rows = min(512, npts)
    block_count = npts // block_rows
    all_index = jnp.arange(npts, dtype=jnp.int32)
    degree_f = degree.astype(jnp.float32)

    def apply(vectors):
        sending = vectors.astype(jnp.bfloat16).astype(jnp.float32)

        def one_block(block_index):
            first_row = (block_index * block_rows).astype(jnp.int32)
            row_points = lax.dynamic_slice_in_dim(points_f, first_row, block_rows, 0)
            row_norms = lax.dynamic_slice_in_dim(sqnorm, first_row, block_rows, 0)
            gram = jnp.dot(row_points, points_f.T, precision=lax.Precision.HIGHEST)
            distance = row_norms[:, None] + sqnorm[None, :] - 2.0 * gram
            kernel = jnp.exp(-sharpness * distance)
            row_index = first_row + jnp.arange(block_rows, dtype=jnp.int32)
            kernel = jnp.where(row_index[:, None] == all_index[None, :], jnp.float32(0.0), kernel)
            kernel = lax.optimization_barrier(kernel.astype(jnp.bfloat16)).astype(jnp.float32)
            return jnp.dot(sending, kernel.T, precision=lax.Precision.HIGHEST)

        blocks = lax.map(one_block, jnp.arange(block_count, dtype=jnp.int32))
        return jnp.transpose(blocks, (1, 0, 2)).reshape(vectors.shape[0], npts)

    vectors = start_vectors.astype(jnp.float32)
    for iteration in range(ITERS):
        vectors = apply(vectors) / degree_f[None, :]
    mean_abs = jnp.sum(jnp.abs(vectors), axis=1) / npts
    return vectors / (mean_abs[:, None] + 1e-6)
```

```python
import jax
import jax.numpy as jnp
from jax import lax
from jax.sharding import PartitionSpec as P

ITERS = 3


def general(points, start_vectors, degree):
    row_count = lax.axis_size("rows")
    col_count = lax.axis_size("cols")
    row_place = lax.axis_index("rows")
    col_place = lax.axis_index("cols")
    span_size = points.shape[0]
    sharpness = 4.0 / points.shape[1]
    row_points, row_degree = (
        lax.all_gather(points, "cols", axis=0, tiled=True),
        lax.all_gather(degree, "cols", axis=0, tiled=True),
    )
    row_total = row_points.shape[0]
    row_float = row_points.astype(jnp.float32)
    row_norms = jnp.sum(row_float * row_float, axis=1)
    row_slots = jnp.arange(row_total, dtype=jnp.int32)
    row_global = (
        row_place * col_count + row_slots // span_size
    ) * span_size + row_slots % span_size
    x_piece = lax.all_gather(points, "rows", axis=0, tiled=True)

    def kernel_block(x_block, col_norms, first_slot):
        inner = lax.dot_general(
            row_points, x_block, (((1,), (1,)), ((), ())), preferred_element_type=jnp.float32
        )
        distance = row_norms[:, None] + col_norms[None, :] - 2.0 * inner
        kernel = jnp.exp(-sharpness * distance)
        col_slots = first_slot + jnp.arange(x_block.shape[0], dtype=jnp.int32)
        col_global = (
            col_slots // span_size * col_count + col_place
        ) * span_size + col_slots % span_size
        return jnp.where(
            row_global[:, None] == col_global[None, :], jnp.float32(0.0), kernel
        ).astype(jnp.bfloat16)

    vectors = start_vectors
    for iteration in range(ITERS):
        empty = jnp.zeros((vectors.shape[0], row_total), jnp.float32)
        sending = vectors.T.astype(jnp.bfloat16)
        v_piece = lax.all_gather(sending, "rows", axis=0, tiled=True)
        piece_rows = x_piece.shape[0]
        block_size = span_size * min(4, row_count)
        block_count = piece_rows // block_size

        def accumulate(block_index, running):
            offset = block_index * block_size
            x_block = lax.dynamic_slice_in_dim(x_piece, offset, block_size, 0)
            v_block = lax.dynamic_slice_in_dim(v_piece, offset, block_size, 0)
            x_float = x_block.astype(jnp.float32)
            col_norms = jnp.sum(x_float * x_float, axis=1)
            kernel = kernel_block(x_block, col_norms, offset)
            return running + lax.dot_general(
                v_block, kernel, (((0,), (1,)), ((), ())), preferred_element_type=jnp.float32
            )

        partial_value = lax.fori_loop(0, block_count, accumulate, empty)
        summed = lax.psum(partial_value, "cols")
        row_state = summed / row_degree.astype(jnp.float32)[None, :]
        vectors = lax.dynamic_slice_in_dim(row_state, col_place * span_size, span_size, 1)
    magnitude = lax.psum(jnp.sum(jnp.abs(row_state), axis=1), "rows")
    mean_abs = magnitude / (span_size * row_count * col_count)
    return vectors / (mean_abs[:, None] + 1e-06)


def swap(value, axis, bit):
    count = lax.axis_size(axis)
    return lax.ppermute(value, axis, [(place, place ^ bit) for place in range(count)])


def planes(points, start_vectors, degree):
    row_count = lax.axis_size("rows")
    span, features = points.shape
    vector_count = start_vectors.shape[0]
    sharpness = 4.0 / features
    extra = jnp.concatenate(
        [
            start_vectors.astype(jnp.bfloat16),
            jnp.broadcast_to(degree[None, :], (vector_count, span)),
        ],
        axis=1,
    )
    message = jnp.concatenate([points, extra], axis=0)
    pieces = [message] + [swap(message, "rows", bit) for bit in range(2, row_count, 2)]
    own = jnp.stack(pieces)
    by_x = swap(own, "cols", 2)
    by_y = swap(own, "rows", 1)
    by_core = swap(own, "cols", 1)
    by_x_core = swap(by_x, "cols", 1)

    def unpack(parts):
        whole = jnp.concatenate(parts, axis=0)
        x = whole[:, :span, :].reshape(-1, features)
        v = jnp.transpose(whole[:, span:, :span], (1, 0, 2)).reshape(vector_count, -1)
        d = whole[:, span, span:].reshape(1, -1)
        return x, v, d.astype(jnp.float32)

    row_x, row_v, row_degree = unpack([own, by_x, by_core, by_x_core])
    col_x, _, col_degree = unpack([own, by_y])

    def norms(x):
        f = x.astype(jnp.float32)
        return jnp.sum(f * f, axis=1)

    inner = lax.dot_general(
        row_x, col_x, (((1,), (1,)), ((), ())), preferred_element_type=jnp.float32
    )
    distance = norms(row_x)[:, None] + norms(col_x)[None, :] - 2.0 * inner
    kernel = jnp.exp(-sharpness * distance)
    row_slot = jnp.arange(row_x.shape[0], dtype=jnp.int32)
    col_slot = jnp.arange(col_x.shape[0], dtype=jnp.int32)
    block = own.shape[0] * span
    diagonal = (row_slot[:, None] == col_slot[None, :]) & (row_slot < block)[:, None]
    kernel = jnp.where(diagonal, jnp.float32(0.0), kernel).astype(jnp.bfloat16)
    kernel = lax.optimization_barrier(kernel)

    def to_cols(v):
        part = lax.dot_general(
            v, kernel, (((1,), (0,)), ((), ())), preferred_element_type=jnp.float32
        )
        other = swap(part, "rows", 1)
        other = jnp.concatenate([other[:, block:], other[:, :block]], axis=1)
        return (part + other) / col_degree

    def to_rows(v):
        part = lax.dot_general(
            v, kernel, (((1,), (1,)), ((), ())), preferred_element_type=jnp.float32
        )
        other = swap(part, "cols", 1)
        part = part + jnp.concatenate([other[:, 2 * block :], other[:, : 2 * block]], axis=1)
        other = swap(part, "cols", 3)
        part = part + jnp.concatenate(
            [other[:, at * block : (at + 1) * block] for at in (3, 2, 1, 0)], axis=1
        )
        return part / row_degree

    state = to_cols(row_v)
    state = to_rows(state.astype(jnp.bfloat16))
    state = to_cols(state.astype(jnp.bfloat16))
    magnitude = jnp.sum(jnp.abs(state), axis=1, keepdims=True)
    magnitude = jnp.broadcast_to(magnitude, (vector_count, span))
    magnitude = magnitude + swap(magnitude, "cols", 1)
    magnitude = magnitude + swap(magnitude, "cols", 3)
    mean_abs = magnitude / (span * row_count * lax.axis_size("cols"))
    return state[:, :span] / (mean_abs + 1e-06)


def solution(mesh):
    small = mesh.shape["cols"] == 4 and mesh.shape["rows"] % 2 == 0 and mesh.shape["rows"] <= 8
    return jax.shard_map(
        planes if small else general,
        mesh=mesh,
        in_specs=(P(("rows", "cols"), None), P(None, ("rows", "cols")), P(("rows", "cols"))),
        out_specs=P(None, ("rows", "cols")),
        check_vma=False,
    )
```

```python
import functools
import math

import jax
import jax.numpy as jnp
from jax import lax
from jax.experimental import pallas as pl
from jax.experimental.pallas import tpu as pltpu
from jax.sharding import PartitionSpec as P

ITERS = 3


def general(points, start_vectors, degree):
    row_count = lax.axis_size("rows")
    col_count = lax.axis_size("cols")
    row_place = lax.axis_index("rows")
    col_place = lax.axis_index("cols")
    span_size = points.shape[0]
    sharpness = 4.0 / points.shape[1]
    row_points, row_degree = (
        lax.all_gather(points, "cols", axis=0, tiled=True),
        lax.all_gather(degree, "cols", axis=0, tiled=True),
    )
    row_total = row_points.shape[0]
    row_float = row_points.astype(jnp.float32)
    row_norms = jnp.sum(row_float * row_float, axis=1)
    row_slots = jnp.arange(row_total, dtype=jnp.int32)
    row_global = (
        row_place * col_count + row_slots // span_size
    ) * span_size + row_slots % span_size
    x_piece = lax.all_gather(points, "rows", axis=0, tiled=True)

    def kernel_block(x_block, col_norms, first_slot):
        inner = lax.dot_general(
            row_points, x_block, (((1,), (1,)), ((), ())), preferred_element_type=jnp.float32
        )
        distance = row_norms[:, None] + col_norms[None, :] - 2.0 * inner
        kernel = jnp.exp(-sharpness * distance)
        col_slots = first_slot + jnp.arange(x_block.shape[0], dtype=jnp.int32)
        col_global = (
            col_slots // span_size * col_count + col_place
        ) * span_size + col_slots % span_size
        return jnp.where(
            row_global[:, None] == col_global[None, :], jnp.float32(0.0), kernel
        ).astype(jnp.bfloat16)

    vectors = start_vectors
    for iteration in range(ITERS):
        empty = jnp.zeros((vectors.shape[0], row_total), jnp.float32)
        sending = vectors.T.astype(jnp.bfloat16)
        v_piece = lax.all_gather(sending, "rows", axis=0, tiled=True)
        piece_rows = x_piece.shape[0]
        block_size = span_size * min(4, row_count)
        block_count = piece_rows // block_size

        def accumulate(block_index, running):
            offset = block_index * block_size
            x_block = lax.dynamic_slice_in_dim(x_piece, offset, block_size, 0)
            v_block = lax.dynamic_slice_in_dim(v_piece, offset, block_size, 0)
            x_float = x_block.astype(jnp.float32)
            col_norms = jnp.sum(x_float * x_float, axis=1)
            kernel = kernel_block(x_block, col_norms, offset)
            return running + lax.dot_general(
                v_block, kernel, (((0,), (1,)), ((), ())), preferred_element_type=jnp.float32
            )

        partial_value = lax.fori_loop(0, block_count, accumulate, empty)
        summed = lax.psum(partial_value, "cols")
        row_state = summed / row_degree.astype(jnp.float32)[None, :]
        vectors = lax.dynamic_slice_in_dim(row_state, col_place * span_size, span_size, 1)
    magnitude = lax.psum(jnp.sum(jnp.abs(row_state), axis=1), "rows")
    mean_abs = magnitude / (span_size * row_count * col_count)
    return vectors / (mean_abs[:, None] + 1e-06)


def swap(value, axis, bit):
    count = lax.axis_size(axis)
    return lax.ppermute(value, axis, [(place, place ^ bit) for place in range(count)])


def call(body, outs, args, flops):
    moved = sum(a.size * a.dtype.itemsize for a in args)
    return pl.pallas_call(
        body,
        out_shape=outs,
        in_specs=[pl.BlockSpec(memory_space=pltpu.VMEM)] * len(args),
        out_specs=jax.tree.map(lambda _: pl.BlockSpec(memory_space=pltpu.VMEM), outs),
        compiler_params=pltpu.CompilerParams(vmem_limit_bytes=16 * 2**20),
        cost_estimate=pl.CostEstimate(flops=flops, bytes_accessed=moved, transcendentals=0),
    )(*args)


def dot(left, right, left_dim, right_dim):
    return lax.dot_general(
        left,
        right,
        (((left_dim,), (right_dim,)), ((), ())),
        preferred_element_type=jnp.float32,
    )


def pack(scale, p_ref, v_ref, d_ref, out_ref):
    span = p_ref.shape[0]
    count = v_ref.shape[0]
    x = p_ref[...]
    f = x.astype(jnp.float32)
    squares = f * f
    high = squares.astype(jnp.bfloat16)
    low = (squares - high.astype(jnp.float32)).astype(jnp.bfloat16)
    ones = jnp.ones((count, x.shape[1]), jnp.bfloat16)
    norm = (dot(ones, high, 1, 1) + dot(ones, low, 1, 1)) * scale
    first = norm.astype(jnp.bfloat16).astype(jnp.float32)
    second = (norm - first).astype(jnp.bfloat16).astype(jnp.float32)
    third = norm - first - second
    place = lax.broadcasted_iota(jnp.int32, norm.shape, 0)
    degree = jnp.broadcast_to(d_ref[...].astype(jnp.float32), norm.shape)
    side = jnp.where(place == 0, degree, jnp.where(place == 1, first, jnp.where(place == 2, second, third)))
    out_ref[:span, :] = x
    out_ref[span:, :span] = v_ref[...].astype(jnp.bfloat16)
    out_ref[span:, span:] = side.astype(jnp.bfloat16)


class Piece:
    def __init__(self, ref, at):
        self.ref, self.at = ref, at
        self.span = ref.shape[1] - 8

    def points(self):
        return self.ref[self.at, : self.span, :]

    def vectors(self):
        return self.ref[self.at, self.span :, : self.span]

    def side(self):
        return self.ref[self.at, self.span :, self.span :].astype(jnp.float32)

    def norm(self):
        side = self.side()
        return side[1:2] + side[2:3] + side[3:4]

    def degree(self):
        return self.side()[0:1]


def pieces(refs):
    return [Piece(ref, at) for ref in refs for at in range(ref.shape[0])]


def wide(parts):
    return jnp.concatenate(parts, axis=1)


def fill(scale, rows, cols, out_ref, same=0):
    span = rows[0].span
    step = 2
    for j in range(0, len(cols), step):
        group = cols[j : j + step]
        x = jnp.concatenate([c.points() for c in group], axis=0)
        bias = wide([c.norm() for c in group])
        for i, row in enumerate(rows):
            tall = jnp.transpose(jnp.broadcast_to(row.norm(), (8, span)))[:, :1]
            inner = dot(row.points(), x, 1, 1)
            value = jnp.exp2(inner * (2.0 * scale) - bias - tall)
            for k in range(len(group)):
                if i == j + k < same:
                    r = lax.broadcasted_iota(jnp.int32, value.shape, 0)
                    c = lax.broadcasted_iota(jnp.int32, value.shape, 1)
                    value = jnp.where(c == r + k * span, 0.0, value)
            out_ref[i * span : (i + 1) * span, j * span : (j + len(group)) * span] = value.astype(
                jnp.bfloat16
            )


def early(scale, sa, sb, ka, kb, xa, xka, ya, out_ref, part_ref):
    rows = pieces([sa, sb, ka, kb, xa, xka])
    cols = pieces([sa, sb, ya])
    fill(scale, rows, cols, out_ref, sa.shape[0] + sb.shape[0])
    part_ref[...] = dot(wide([r.vectors() for r in rows]), out_ref[...], 1, 0)


def middle(scale, sa, sb, ka, kb, xa, xka, ya, xb, yb, part1, out_y, out_x, part_ref):
    rows = pieces([sa, sb, ka, kb, xa, xka])
    late = pieces([xb])
    fill(scale, rows, pieces([yb]), out_y)
    fill(scale, late, pieces([sa, sb, ya, yb]), out_x)
    split = part1.shape[1]
    part = dot(wide([r.vectors() for r in late]), out_x[...], 1, 0)
    part_ref[:, :split] = part1[...] + part[:, :split]
    part_ref[:, split:] = dot(wide([r.vectors() for r in rows]), out_y[...], 1, 0) + part[:, split:]


def last(scale, sa, sb, ya, yb, xkb, part2, out_k, part_ref):
    late = pieces([xkb])
    fill(scale, late, pieces([sa, sb, ya, yb]), out_k)
    part_ref[...] = part2[...] + dot(wide([r.vectors() for r in late]), out_k[...], 1, 0)


def order(value, places, size):
    return wide([value[:, p * size : (p + 1) * size] for p in places])


def to_rows(sa, sb, ya, yb, a1, ay, ax, ak, part, other, out_ref):
    degree = wide([c.degree() for c in pieces([sa, sb, ya, yb])])
    block = degree.shape[1] // 4
    state = (part[...] + order(other[...], (2, 3, 0, 1), block)) / degree
    v = state.astype(jnp.bfloat16)
    split = a1.shape[1]
    r1 = a1.shape[0]
    r2 = r1 + ax.shape[0]
    out_ref[:, :r1] = dot(v[:, :split], a1[...], 1, 1) + dot(v[:, split:], ay[...], 1, 1)
    out_ref[:, r1:r2] = dot(v, ax[...], 1, 1)
    out_ref[:, r2:] = dot(v, ak[...], 1, 1)


def to_cols(sa, sb, ka, kb, xa, xka, xb, xkb, a1, ay, ax, ak, part, other, out_ref):
    degree = wide([c.degree() for c in pieces([sa, sb, ka, kb, xa, xka, xb, xkb])])
    block = degree.shape[1] // 8
    state = (part[...] + order(other[...], (5, 7, 4, 6, 2, 0, 3, 1), block)) / degree
    v = state.astype(jnp.bfloat16)
    split = a1.shape[1]
    r1 = a1.shape[0]
    r2 = r1 + ax.shape[0]
    tail = dot(v[:, r1:r2], ax[...], 1, 0) + dot(v[:, r2:], ak[...], 1, 0)
    out_ref[:, :split] = dot(v[:, :r1], a1[...], 1, 0) + tail[:, :split]
    out_ref[:, split:] = dot(v[:, :r1], ay[...], 1, 0) + tail[:, split:]


def finish(sa, sb, ya, yb, part, other, own_ref, sum_ref):
    degree = wide([c.degree() for c in pieces([sa, sb, ya, yb])])
    block = degree.shape[1] // 4
    state = (part[...] + order(other[...], (2, 3, 0, 1), block)) / degree
    own_ref[...] = state[:, : own_ref.shape[1]]
    total = jnp.sum(jnp.abs(state), axis=1, keepdims=True)
    sum_ref[...] = jnp.broadcast_to(total, sum_ref.shape)


def planes(points, start_vectors, degree):
    row_count = lax.axis_size("rows")
    span, features = points.shape
    count = start_vectors.shape[0]
    scale = 4.0 / features * math.log2(math.e)

    def shape(rows, cols, kind=jnp.float32):
        return jax.ShapeDtypeStruct((rows, cols), kind)

    message = call(
        functools.partial(pack, scale),
        shape(span + 8, features, jnp.bfloat16),
        (points, start_vectors, degree[None, :]),
        10**6,
    )
    remote = [swap(message, "rows", bit) for bit in range(2, row_count, 2)]
    sa = jnp.stack([message, remote[0]])
    sb = jnp.stack(remote[1:])
    xa, ya, ka = swap(sa, "cols", 2), swap(sa, "rows", 1), swap(sa, "cols", 1)
    xb, yb, kb = swap(sb, "cols", 2), swap(sb, "rows", 1), swap(sb, "cols", 1)
    xka, xkb = swap(xa, "cols", 1), swap(xb, "cols", 1)

    half = sa.shape[0] * span
    rest = sb.shape[0] * span
    r1 = 4 * half + 2 * rest
    split = 2 * half + rest
    width = split + rest
    a1, part1 = call(
        functools.partial(early, scale),
        (shape(r1, split, jnp.bfloat16), shape(count, split)),
        (sa, sb, ka, kb, xa, xka, ya),
        2 * features * r1 * split,
    )
    ay, ax, part2 = call(
        functools.partial(middle, scale),
        (shape(r1, rest, jnp.bfloat16), shape(rest, width, jnp.bfloat16), shape(count, width)),
        (sa, sb, ka, kb, xa, xka, ya, xb, yb, part1),
        2 * features * (r1 * rest + rest * width),
    )
    ak, part = call(
        functools.partial(last, scale),
        (shape(rest, width, jnp.bfloat16), shape(count, width)),
        (sa, sb, ya, yb, xkb, part2),
        2 * features * rest * width,
    )
    part = call(
        to_rows,
        shape(count, r1 + 2 * rest),
        (sa, sb, ya, yb, a1, ay, ax, ak, part, swap(part, "rows", 1)),
        10**8,
    )
    part = part + order(swap(part, "cols", 1), (2, 3, 0, 1, 5, 4, 7, 6), rest)
    part = call(
        to_cols,
        shape(count, width),
        (sa, sb, ka, kb, xa, xka, xb, xkb, a1, ay, ax, ak, part, swap(part, "cols", 3)),
        10**8,
    )
    own, total = call(
        finish,
        (shape(count, span), shape(count, span)),
        (sa, sb, ya, yb, part, swap(part, "rows", 1)),
        10**6,
    )
    total = total + swap(total, "cols", 1)
    total = total + swap(total, "cols", 3)
    mean_abs = total / (span * row_count * lax.axis_size("cols"))
    return own / (mean_abs + 1e-06)


def solution(mesh):
    small = mesh.shape["cols"] == 4 and mesh.shape["rows"] == 8
    return jax.shard_map(
        planes if small else general,
        mesh=mesh,
        in_specs=(P(("rows", "cols"), None), P(None, ("rows", "cols")), P(("rows", "cols"))),
        out_specs=P(None, ("rows", "cols")),
        check_vma=False,
    )
```

```python
import functools
import math

import jax
import jax.numpy as jnp
from jax import lax
from jax.experimental import pallas as pl
from jax.experimental.pallas import tpu as pltpu
from jax.sharding import PartitionSpec as P


ITERS = 3


def general(points, start_vectors, degree):
    row_count = lax.axis_size("rows")
    col_count = lax.axis_size("cols")
    row_place = lax.axis_index("rows")
    col_place = lax.axis_index("cols")
    span_size = points.shape[0]
    sharpness = 4.0 / points.shape[1]
    row_points, row_degree = (
        lax.all_gather(points, "cols", axis=0, tiled=True),
        lax.all_gather(degree, "cols", axis=0, tiled=True),
    )
    row_total = row_points.shape[0]
    row_float = row_points.astype(jnp.float32)
    row_norms = jnp.sum(row_float * row_float, axis=1)
    row_slots = jnp.arange(row_total, dtype=jnp.int32)
    row_global = (
        row_place * col_count + row_slots // span_size
    ) * span_size + row_slots % span_size
    x_piece = lax.all_gather(points, "rows", axis=0, tiled=True)

    def kernel_block(x_block, col_norms, first_slot):
        inner = lax.dot_general(
            row_points, x_block, (((1,), (1,)), ((), ())), preferred_element_type=jnp.float32
        )
        distance = row_norms[:, None] + col_norms[None, :] - 2.0 * inner
        kernel = jnp.exp(-sharpness * distance)
        col_slots = first_slot + jnp.arange(x_block.shape[0], dtype=jnp.int32)
        col_global = (
            col_slots // span_size * col_count + col_place
        ) * span_size + col_slots % span_size
        return jnp.where(
            row_global[:, None] == col_global[None, :], jnp.float32(0.0), kernel
        ).astype(jnp.bfloat16)

    vectors = start_vectors
    for _ in range(ITERS):
        empty = jnp.zeros((vectors.shape[0], row_total), jnp.float32)
        sending = vectors.T.astype(jnp.bfloat16)
        v_piece = lax.all_gather(sending, "rows", axis=0, tiled=True)
        piece_rows = x_piece.shape[0]
        block_size = span_size * min(4, row_count)
        block_count = piece_rows // block_size

        def accumulate(block_index, running):
            offset = block_index * block_size
            x_block = lax.dynamic_slice_in_dim(x_piece, offset, block_size, 0)
            v_block = lax.dynamic_slice_in_dim(v_piece, offset, block_size, 0)
            x_float = x_block.astype(jnp.float32)
            col_norms = jnp.sum(x_float * x_float, axis=1)
            kernel = kernel_block(x_block, col_norms, offset)
            return running + lax.dot_general(
                v_block, kernel, (((0,), (1,)), ((), ())), preferred_element_type=jnp.float32
            )

        partial_value = lax.fori_loop(0, block_count, accumulate, empty)
        summed = lax.psum(partial_value, "cols")
        row_state = summed / row_degree.astype(jnp.float32)[None, :]
        vectors = lax.dynamic_slice_in_dim(row_state, col_place * span_size, span_size, 1)
    magnitude = lax.psum(jnp.sum(jnp.abs(row_state), axis=1), "rows")
    mean_abs = magnitude / (span_size * row_count * col_count)
    return vectors / (mean_abs[:, None] + 1e-06)


def swap(value, row_bit, col_bit):
    cols = lax.axis_size("cols")
    count = lax.axis_size("rows") * cols
    bits = row_bit * cols + col_bit
    return lax.ppermute(value, ("rows", "cols"), [(place, place ^ bits) for place in range(count)])


def call(body, outs, args, flops):
    moved = sum(a.size * a.dtype.itemsize for a in args)
    return inner_call(body, outs, args, flops, moved)


def inner_call(body, outs, args, flops, moved):
    return pl.pallas_call(
        body,
        out_shape=outs,
        in_specs=[pl.BlockSpec(memory_space=pltpu.VMEM)] * len(args),
        out_specs=jax.tree.map(lambda _: pl.BlockSpec(memory_space=pltpu.VMEM), outs),
        compiler_params=pltpu.CompilerParams(vmem_limit_bytes=16 * 2**20),
        cost_estimate=pl.CostEstimate(flops=flops, bytes_accessed=moved, transcendentals=0),
    )(*args)


def dot(left, right, left_dim, right_dim):
    return lax.dot_general(
        left,
        right,
        (((left_dim,), (right_dim,)), ((), ())),
        preferred_element_type=jnp.float32,
    )


def pack(scale, p_any, v_any, d_any, out_ref, p_ref, v_ref, d_ref, sems):
    span = p_ref.shape[0]
    copies = [
        pltpu.make_async_copy(source, target, sems.at[at])
        for at, (source, target) in enumerate(((p_any, p_ref), (v_any, v_ref), (d_any, d_ref)))
    ]
    for copy in copies:
        copy.start()
    for copy in copies:
        copy.wait()
    count = v_ref.shape[0]
    x = p_ref[...]
    f = x.astype(jnp.float32)
    squares = f * f
    high = squares.astype(jnp.bfloat16)
    low = (squares - high.astype(jnp.float32)).astype(jnp.bfloat16)
    ones = jnp.ones((count, x.shape[1]), jnp.bfloat16)
    norm = (dot(ones, high, 1, 1) + dot(ones, low, 1, 1)) * scale
    first = norm.astype(jnp.bfloat16).astype(jnp.float32)
    second = (norm - first).astype(jnp.bfloat16).astype(jnp.float32)
    third = norm - first - second
    place = lax.broadcasted_iota(jnp.int32, norm.shape, 0)
    degree = jnp.broadcast_to(d_ref[...].astype(jnp.float32), norm.shape)
    side = jnp.where(place == 0, degree, jnp.where(place == 1, first, jnp.where(place == 2, second, third)))
    out_ref[:span, :] = x
    out_ref[span:, :span] = v_ref[...].astype(jnp.bfloat16)
    out_ref[span:, span:] = side.astype(jnp.bfloat16)


class Piece:
    def __init__(self, ref, at):
        self.ref, self.at = ref, at
        self.span = ref.shape[1] - 8

    def points(self):
        return self.ref[self.at, : self.span, :]

    def vectors(self):
        return self.ref[self.at, self.span :, : self.span]

    def side(self):
        return self.ref[self.at, self.span :, self.span :].astype(jnp.float32)

    def norm(self):
        side = self.side()
        return side[1:2] + side[2:3] + side[3:4]

    def degree(self):
        return self.side()[0:1]


def pieces(refs):
    return [Piece(ref, at) for ref in refs for at in range(ref.shape[0])]


def wide(parts):
    return jnp.concatenate(parts, axis=1)


def fill(scale, rows, cols, out_ref, same=0):
    span = rows[0].span
    step = 2
    for j in range(0, len(cols), step):
        group = cols[j : j + step]
        x = jnp.concatenate([c.points() for c in group], axis=0)
        bias = wide([c.norm() for c in group])
        for i, row in enumerate(rows):
            tall = jnp.transpose(jnp.broadcast_to(row.norm(), (8, span)))[:, :1]
            inner = dot(row.points(), x, 1, 1)
            value = jnp.exp2(inner * (2.0 * scale) - bias - tall)
            for k in range(len(group)):
                if i == j + k < same:
                    r = lax.broadcasted_iota(jnp.int32, value.shape, 0)
                    c = lax.broadcasted_iota(jnp.int32, value.shape, 1)
                    value = jnp.where(c == r + k * span, 0.0, value)
            out_ref[i * span : (i + 1) * span, j * span : (j + len(group)) * span] = value.astype(
                jnp.bfloat16
            )


def early(scale, sa, sb, ka, kb, xa, xka, ya, out_ref, part_ref):
    rows = pieces([sa, sb, ka, kb, xa, xka])
    cols = pieces([sa, sb, ya])
    fill(scale, rows, cols, out_ref, sa.shape[0] + sb.shape[0])
    part_ref[...] = dot(wide([r.vectors() for r in rows]), out_ref[...], 1, 0)


def middle(scale, sa, sb, ka, kb, xa, xka, ya, xkb, yb, part1, out_y, out_x, part_ref):
    rows = pieces([sa, sb, ka, kb, xa, xka])
    late = pieces([xkb])
    fill(scale, rows, pieces([yb]), out_y)
    fill(scale, late, pieces([sa, sb, ya, yb]), out_x)
    split = part1.shape[1]
    part = dot(wide([r.vectors() for r in late]), out_x[...], 1, 0)
    part_ref[:, :split] = part1[...] + part[:, :split]
    part_ref[:, split:] = dot(wide([r.vectors() for r in rows]), out_y[...], 1, 0) + part[:, split:]


def last(scale, sa, sb, ya, yb, xb, part2, out_k, part_ref):
    late = pieces([xb])
    fill(scale, late, pieces([sa, sb, ya, yb]), out_k)
    part_ref[...] = part2[...] + dot(wide([r.vectors() for r in late]), out_k[...], 1, 0)


def order(value, places, size):
    return wide([value[:, p * size : (p + 1) * size] for p in places])


def to_rows(sa, sb, ya, yb, a1, ay, ax, ak, part, other, out_ref):
    degree = wide([c.degree() for c in pieces([sa, sb, ya, yb])])
    block = degree.shape[1] // 4
    state = (part[...] + order(other[...], (2, 3, 0, 1), block)) / degree
    v = state.astype(jnp.bfloat16)
    split = a1.shape[1]
    r1 = a1.shape[0]
    r2 = r1 + ax.shape[0]
    out_ref[:, :r1] = dot(v[:, :split], a1[...], 1, 1) + dot(v[:, split:], ay[...], 1, 1)
    out_ref[:, r1:r2] = dot(v, ax[...], 1, 1)
    out_ref[:, r2:] = dot(v, ak[...], 1, 1)


def to_cols(sa, sb, ka, kb, xa, xka, xkb, xb, a1, ay, ax, ak, part, other, out_ref):
    degree = wide([c.degree() for c in pieces([sa, sb, ka, kb, xa, xka, xkb, xb])])
    block = degree.shape[1] // 8
    state = (part[...] + order(other[...], (5, 6, 4, 7, 2, 0, 1, 3), block)) / degree
    v = state.astype(jnp.bfloat16)
    split = a1.shape[1]
    r1 = a1.shape[0]
    r2 = r1 + ax.shape[0]
    tail = dot(v[:, r1:r2], ax[...], 1, 0) + dot(v[:, r2:], ak[...], 1, 0)
    out_ref[:, :split] = dot(v[:, :r1], a1[...], 1, 0) + tail[:, :split]
    out_ref[:, split:] = dot(v[:, :r1], ay[...], 1, 0) + tail[:, split:]


def finish(sa, sb, ya, yb, part, other, own_ref, sum_ref):
    degree = wide([c.degree() for c in pieces([sa, sb, ya, yb])])
    block = degree.shape[1] // 4
    state = (part[...] + order(other[...], (2, 3, 0, 1), block)) / degree
    own_ref[...] = state[:, : own_ref.shape[1]]
    total = jnp.sum(jnp.abs(state), axis=1, keepdims=True)
    sum_ref[...] = jnp.broadcast_to(total, sum_ref.shape)


def planes(points, start_vectors, degree):
    row_count = lax.axis_size("rows")
    span, features = points.shape
    count = start_vectors.shape[0]
    scale = 4.0 / features * math.log2(math.e)

    def shape(rows, cols, kind=jnp.float32):
        return jax.ShapeDtypeStruct((rows, cols), kind)

    inputs = (points, start_vectors, degree[None, :])
    message = pl.pallas_call(
        functools.partial(pack, scale),
        out_shape=shape(span + 8, features, jnp.bfloat16),
        in_specs=[pl.BlockSpec(memory_space=pltpu.HBM)] * 3,
        out_specs=pl.BlockSpec(memory_space=pltpu.VMEM),
        scratch_shapes=[pltpu.VMEM(a.shape, a.dtype) for a in inputs]
        + [pltpu.SemaphoreType.DMA((3,))],
        compiler_params=pltpu.CompilerParams(vmem_limit_bytes=16 * 2**20),
    )(*inputs)
    z3 = swap(message, 6, 1)
    z2 = swap(message, 4, 1)
    z1 = swap(message, 2, 1)
    sa = jnp.stack([message, z1])
    sb = jnp.stack([z2, z3])
    xka, ya, ka = swap(sa, 0, 3), swap(sa, 1, 1), swap(sa, 0, 1)
    xkb, yb, kb = swap(sb, 0, 3), swap(sb, 1, 1), swap(sb, 0, 1)
    xa, xb = swap(xka, 0, 1), swap(xkb, 0, 1)

    half = sa.shape[0] * span
    rest = sb.shape[0] * span
    r1 = 4 * half + 2 * rest
    split = 2 * half + rest
    width = split + rest
    a1, part1 = call(
        functools.partial(early, scale),
        (shape(r1, split, jnp.bfloat16), shape(count, split)),
        (sa, sb, ka, kb, xa, xka, ya),
        2 * features * r1 * split,
    )
    ay, ax, part2 = call(
        functools.partial(middle, scale),
        (shape(r1, rest, jnp.bfloat16), shape(rest, width, jnp.bfloat16), shape(count, width)),
        (sa, sb, ka, kb, xa, xka, ya, xkb, yb, part1),
        2 * features * (r1 * rest + rest * width),
    )
    ak, part = call(
        functools.partial(last, scale),
        (shape(rest, width, jnp.bfloat16), shape(count, width)),
        (sa, sb, ya, yb, xb, part2),
        2 * features * rest * width,
    )
    part = call(
        to_rows,
        shape(count, r1 + 2 * rest),
        (sa, sb, ya, yb, a1, ay, ax, ak, part, swap(part, 1, 1)),
        10**8,
    )
    part = part + order(swap(part, 0, 1), (2, 3, 0, 1, 5, 4, 7, 6), rest)
    part = call(
        to_cols,
        shape(count, width),
        (sa, sb, ka, kb, xa, xka, xkb, xb, a1, ay, ax, ak, part, swap(part, 0, 3)),
        10**8,
    )
    own, total = call(
        finish,
        (shape(count, span), shape(count, span)),
        (sa, sb, ya, yb, part, swap(part, 1, 1)),
        10**6,
    )
    total = total + swap(total, 0, 1)
    total = total + swap(total, 0, 3)
    mean_abs = total / (span * row_count * lax.axis_size("cols"))
    return own / (mean_abs + 1e-06)


def solution(mesh):
    specs = dict(
        mesh=mesh,
        in_specs=(P(("rows", "cols"), None), P(None, ("rows", "cols")), P(("rows", "cols"))),
        out_specs=P(None, ("rows", "cols")),
        check_vma=False,
    )
    if mesh.shape["cols"] != 4 or mesh.shape["rows"] != 8:
        return jax.shard_map(general, **specs)

    return jax.shard_map(planes, **specs)
```
